32 devices in a mesh: gx: 16 (over z, y, core), gy: 2 (over x).
Axes of the slice: x: 2, y: 2, z: 4, core: 2. Of those that a mesh axis runs over, the one named last changes fastest.
Arguments:
- old_block: float32 [12288, 24576], P('gx', 'gy'), may hold values from -6 to 6
- vectors: bfloat16 [256, 2, 12288], P(None, 'gy', 'gx'), may hold values from -4 to 4
- prior: bfloat16 [32768, 3072], P('gx', 'gy'), may hold values from -2 to 2
- pair_columns: float32 [32768, 128], P(('gx', 'gy')), may hold values from -6 to 6
- pivots: int32 [128], replicated, may hold values from 0 to 32767
Outputs:
- new_block: float32 [12288, 24576], P('gx', 'gy')
- residual_columns: float32 [32768, 128], P(('gx', 'gy'))
The draws below stay inside these ranges and needn't reach their ends.
Inputs may be any that keep to these rules, and one draw needn't show every extreme that they name: `pivots`: pivot AO-pair row indices, repeats possible.
All inputs are finite; a program needn't handle non-finite values.
Results may differ from the reference program's by a relative error of at most 0.0055.
Values may be sent and summed in bfloat16 or wider, within the bound.
A program may use at most 192 MiB of HBM per device.

```python
import jax
import jax.numpy as jnp
from jax import lax

NVEC = 256
NPRIOR = 3072
NPIV = 128
NIA = 24576
SLAB = 12288
NPAIR = 32768
N_GY = 2


def plant(entries, stream_key, low, largest):
    longest = entries.shape.index(max(entries.shape))
    spots = []
    for shift in (0, 1):
        where = [jax.random.randint(jax.random.fold_in(stream_key, axis), (), 0, length) for axis, length in enumerate(entries.shape)]
        where[longest] = (where[longest] + shift) % entries.shape[longest]
        spots.append(tuple(where))
    return entries.at[spots[0]].set(low).at[spots[1]].set(largest)


def block_levels(own_key, extent, split, least, largest):
    level = 1.0
    for axis_at, shards_of in split:
        steps = jax.random.uniform(jax.random.fold_in(jax.random.fold_in(own_key, 6), axis_at), (shards_of,), jnp.float32, least / len(split), largest / len(split))
        level = level * jnp.repeat(jnp.exp(steps), extent[axis_at] // shards_of).reshape((-1,) + (1,) * (len(extent) - 1 - axis_at))
    return level


def scatter_about(own_key, extent, deviation, bound, split=(), held_as=jnp.bfloat16):
    drawn = jax.random.normal(own_key, extent, jnp.float32) * deviation
    if len(split) > 0:
        drawn = block_levels(own_key, extent, split, -0.22, 0.18) * drawn
    return jnp.clip(drawn, min=-bound, max=bound).astype(held_as)


def setup_inputs(seed: int = 0) -> dict:
    streams_of = jax.random.split(jax.random.key(seed), 6)
    old_block = scatter_about(streams_of[0], (SLAB, NIA), 1.0, 6.0, ((0, 16), (1, 2)), jnp.float32)
    vectors = scatter_about(streams_of[1], (NVEC, N_GY, NIA // N_GY), (NVEC ** -0.25), 4.0, ((1, 2), (2, 16)))
    prior = scatter_about(streams_of[2], (NPAIR, NPRIOR), (NPRIOR ** -0.25), 2.0, ((0, 16), (1, 2)))
    pair_columns = scatter_about(streams_of[3], (NPAIR, NPIV), 1.0, 6.0, ((0, 32),), jnp.float32)
    pivots = plant(jax.random.randint(streams_of[4], (NPIV,), 0, NPAIR), jax.random.fold_in(streams_of[4], 1), 0, NPAIR - 1).astype(jnp.int32)
    return dict(old_block=old_block, vectors=vectors, prior=prior, pair_columns=pair_columns, pivots=pivots)


def reference(old_block, vectors, prior, pair_columns, pivots):
    flat = vectors.reshape(NVEC, NIA)
    slab = NIA // N_GY
    new_block = old_block + jnp.dot(flat[:, :slab].T, flat, preferred_element_type=jnp.float32)
    picked = jnp.take(prior, pivots, axis=0)
    width = NPRIOR // N_GY
    intersection = jnp.zeros((prior.shape[0], NPIV), jnp.float32)
    for group in range(N_GY):
        part = jnp.dot(prior[:, group * width:(group + 1) * width], picked[:, group * width:(group + 1) * width].T, preferred_element_type=jnp.float32)
        rounded = lax.optimization_barrier(part.astype(jnp.bfloat16))
        intersection = intersection + rounded.astype(jnp.float32)
    return new_block, pair_columns - intersection
```

```python
import functools

import jax
import jax.numpy as jnp
from jax import lax
from jax.experimental import pallas as pl
from jax.experimental.pallas import tpu as pltpu
from jax.sharding import PartitionSpec as P

F32 = jnp.float32
BF16 = jnp.bfloat16
MESH = pl.DeviceIdType.MESH
TILE = 256


def from_root(value, axis, root):
    mine = lax.axis_index(axis) == root
    return lax.psum(jnp.where(mine, value, jnp.zeros_like(value)), axis)


def plain(old_block, vectors, prior, pair_columns, pivots):
    local_vectors = vectors.reshape(vectors.shape[0], vectors.shape[2])
    slab_part = from_root(local_vectors, "gy", 0)
    gained = jnp.dot(slab_part.T, lax.all_gather(local_vectors, "gx", axis=1, tiled=True), preferred_element_type=F32)
    new_block = old_block + gained
    rows_local = prior.shape[0]
    local_index = pivots - lax.axis_index("gx") * rows_local
    inside = jnp.logical_and(local_index >= 0, local_index < rows_local)
    chosen = jnp.take(prior, jnp.clip(local_index, 0, rows_local - 1), axis=0)
    chosen = jnp.where(inside[:, None], chosen, jnp.zeros_like(chosen))
    pivot_block = lax.psum(chosen, "gx")
    part = jnp.dot(prior, pivot_block.T, preferred_element_type=F32).astype(BF16)
    parts = lax.all_to_all(part.reshape(lax.axis_size("gy"), -1, part.shape[1]), "gy", split_axis=0, concat_axis=0)
    rounded = lax.optimization_barrier(parts)
    return new_block, pair_columns - jnp.sum(rounded.astype(F32), axis=0)


def gather_kernel(n, vec_ref, prior_ref, old_ref, pair_ref, piv_ref, acc, resid, held, slab, slab_t, prior, chosen, half_in,
                  half, rs_in, pick, parts, parts_in, vec_sem, prior_sem, old_sem, v_send, v_recv, s_send, s_recv, d_send,
                  d_recv, rs_send, rs_recv, ag_send, ag_recv, p_send, p_recv):
    line, chips = n // 4, n // 2
    chunks = held.shape[1]
    width = chunks * TILE
    keys = piv_ref.shape[1]
    roots, each = pick.shape[1], pick.shape[2]
    rows_of = prior.shape[0] // 2
    gx, gy = lax.axis_index("gx"), lax.axis_index("gy")
    pos, y, core = gx // 4, lax.rem(gx // 2, 2), lax.rem(gx, 2)
    chip = gx // 2
    flip = pos >= line // 2
    mirrored = jnp.where(flip, line - 1 - pos, pos)

    def at(k, yy, c):
        return (jnp.where(flip, line - 1 - k, k) * 2 + yy) * 2 + c

    def vec_copy(ch):
        return pltpu.make_async_copy(vec_ref.at[:, pl.ds(ch * TILE, TILE)], held.at[gx, ch], vec_sem.at[ch])

    for ch in range(chunks):
        vec_copy(ch).start()
    prior_in = pltpu.make_async_copy(prior_ref, prior, prior_sem)
    prior_in.start()

    barrier = pltpu.get_barrier_semaphore()
    for step in range(1, n):
        pl.semaphore_signal(barrier, inc=1, device_id=(lax.rem(gx + step, n), gy), device_id_type=MESH)
    pl.semaphore_signal(barrier, inc=1, device_id=(gx, 1 - gy), device_id_type=MESH)

    def old_copy(src):
        columns = pl.ds(pl.multiple_of(src * width, 128), width)
        return pltpu.make_async_copy(old_ref.at[:, columns], acc.at[:, columns], old_sem.at[src])

    def chunk_copy(src, ch, way, target):
        return pltpu.make_async_remote_copy(held.at[src, ch], held.at[src, ch], v_send.at[src, ch, way], v_recv.at[src, ch], device_id=(target, gy), device_id_type=MESH)

    def slab_copy(ch):
        return pltpu.make_async_remote_copy(held.at[gx, ch], slab.at[ch], s_send.at[ch], s_recv.at[ch], device_id=(gx, 1 - gy), device_id_type=MESH)

    partner = at(jnp.where(flip, line - 1 - pos, pos), y, 1 - core)

    def update(src, first, last):
        def rows_step(i, _):
            rows = pl.ds(pl.multiple_of(i * TILE, TILE), TILE)
            for ch in range(first, last):
                columns = pl.ds(pl.multiple_of(src * width + ch * TILE, TILE), TILE)
                acc[rows, columns] += jnp.dot(slab_t[rows, :], held[src, ch], preferred_element_type=F32)
            return 0
        lax.fori_loop(0, acc.shape[0] // TILE, rows_step, 0)

    def first_swap():
        return pltpu.make_async_remote_copy(chosen.at[1 - core], half_in, d_send.at[0], d_recv.at[0], device_id=(partner, gy), device_id_type=MESH)

    def last_swap(c):
        return pltpu.make_async_remote_copy(pick.at[c], pick.at[c], d_send.at[1], d_recv.at[1], device_id=(partner, gy), device_id_type=MESH)

    def parts_copy():
        return pltpu.make_async_remote_copy(parts.at[1 - gy], parts_in, p_send, p_recv, device_id=(gx, 1 - gy), device_id_type=MESH)

    def root_chip(r):
        return line // 2 * 2 - 2 + r

    def rs_copy(r, sender):
        return pltpu.make_async_remote_copy(half.at[r], rs_in.at[sender], rs_send.at[r], rs_recv.at[sender], device_id=(root_chip(r) * 2 + core, gy), device_id_type=MESH)

    def ag_copy(r, k):
        return pltpu.make_async_remote_copy(pick.at[core, r], pick.at[core, r], ag_send.at[k], ag_recv.at[r], device_id=(k * 2 + core, gy), device_id_type=MESH)

    def run(me):
        end = me == 0
        other = 1 - y
        order, seen, queue, sent = [], set(), [], []

        def send(block, ch, way):
            k, own_y = block
            target = {"down": at(me - 1, y, core), "up": at(me + 1, y, core), "y": at(me, other, core), "core": partner}[way]
            copy = chunk_copy(at(k, y if own_y else other, core), ch, {"down": 0, "up": 1, "y": 2, "core": 3}[way], target)
            copy.start()
            sent.append(copy)

        def landed(block, ch, mine=True):
            k, own_y = block
            src = at(k, y if own_y else other, core if mine else 1 - core)
            chunk_copy(src, ch, 0, gx).wait_recv()

        def ways(block, ch):
            k, own_y = block
            if end:
                out = []
                if block == (0, True):
                    out = ["y", "up"]
                elif block == (0, False):
                    out = ["up"]
                elif own_y and not (k == 1 and ch == chunks - 1):
                    out = ["y"]
                return out + ["core"]
            out = []
            if block == (1, True):
                out = ["down", "up", "y"]
            elif own_y and k > 1:
                out = ["down", "y"]
            elif block == (0, True):
                out = ["up"]
            return out + ["core"]

        if end:
            from_z = [((1, True), c) for c in range(chunks)] + [((2, True), c) for c in range(chunks)] + [((3, True), c) for c in range(chunks)] + [((1, False), chunks - 1)]
            from_y = [((0, False), c) for c in range(chunks)] + [((1, False), c) for c in range(chunks - 1)] + [((2, False), c) for c in range(chunks)] + [((3, False), c) for c in range(chunks)]
            streams = [from_z, from_y]
        else:
            streams = [
                [((2, True), c) for c in range(chunks)] + [((3, True), c) for c in range(chunks)],
                [((0, True), c) for c in range(chunks)] + [((0, False), c) for c in range(chunks)],
                [((k, False), c) for k in (1, 2, 3) for c in range(chunks)],
            ]
        slots = max(len(s) for s in streams)
        own = (me, True)

        for ch in range(chunks):
            vec_copy(ch).wait()
            for way in ways(own, ch):
                if way != "core":
                    send(own, ch, way)
            pl.when(gy == 0)(slab_copy(ch).start)
        for ch in range(chunks):
            send(own, ch, "core")
        prior_in.wait()

        arrivals = [[(own, c) for c in range(chunks)]] + [[s[i] for s in streams if i < len(s)] for i in range(slots)]
        blocks = []
        for group in arrivals:
            for block, _ in group:
                if block not in blocks:
                    blocks.append(block)
        for k, own_y in blocks:
            for c in (core, 1 - core):
                old_copy(at(k, y if own_y else other, c)).start()

        got, ready = {}, []

        def note(block, ch, mine):
            got.setdefault((block, mine), set()).add(ch)
            if len(got[(block, mine)]) == chunks:
                ready.append((block, mine, 0, chunks))

        def compute(count):
            for _ in range(count):
                if not ready:
                    return
                (k, own_y), mine, lo, hi = ready.pop(0)
                src = at(k, y if own_y else other, core if mine else 1 - core)
                if not mine:
                    for ch in range(lo, hi):
                        landed((k, own_y), ch, False)
                old_copy(src).wait()
                update(src, lo, hi)

        def receive(slot):
            for block, ch in arrivals[slot]:
                landed(block, ch)
                for way in ways(block, ch):
                    send(block, ch, way)
                if not end and block == (3, True) and ch == chunks - 1:
                    send((1, False), chunks - 1, "down")
            for mine in (True, False):
                for block, ch in arrivals[slot]:
                    note(block, ch, mine)

        for ch in range(chunks):
            note(own, ch, True)
            note(own, ch, False)

        base = gx * prior.shape[0]
        key = jnp.broadcast_to(piv_ref[...], (keys, keys)).T
        key = key[:, :1] - base
        onehot = (lax.broadcasted_iota(jnp.int32, (keys, prior.shape[0]), 1) == key).astype(F32).astype(BF16)
        portion = keys // 2

        def pick_tile(i, _):
            columns = pl.ds(pl.multiple_of(i * TILE, TILE), TILE)
            got_rows = jnp.dot(onehot, prior[:, columns], preferred_element_type=F32).astype(BF16)
            for c in range(2):
                for r in range(roots):
                    start = c * portion + r * each
                    chosen[c, r, :, columns] = got_rows[start:start + each, :]
            return 0
        lax.fori_loop(0, prior.shape[1] // TILE, pick_tile, 0)

        receive(1)
        first_swap().start()
        first_swap().wait_recv()
        for r in range(roots):
            half[r] = (chosen[core, r].astype(F32) + half_in[r].astype(F32)).astype(BF16)
        receive(2)
        for r in range(roots):
            if end:
                rs_copy(r, chip).start()
            else:
                pl.when(chip != root_chip(r))(rs_copy(r, chip).start)
        receive(3)

        @pl.when(gy == 0)
        def _():
            for ch in range(chunks):
                slab_t[ch * TILE:(ch + 1) * TILE, :] = held[gx, ch].T

        @pl.when(gy != 0)
        def _():
            for ch in range(chunks):
                slab_copy(ch).wait_recv()
                slab_t[ch * TILE:(ch + 1) * TILE, :] = slab[ch].T

        if not end:
            mine = chip - root_chip(0)
            total = half[mine].astype(F32)
            for step in range(1, chips):
                sender = lax.rem(chip + step, chips)
                rs_copy(0, sender).wait_recv()
                total = total + rs_in[sender].astype(F32)
            pick[core, mine] = total.astype(BF16)
        compute(2)
        if not end:
            for step in range(1, chips):
                ag_copy(mine, lax.rem(chip + step, chips)).start()
        receive(4)
        compute(3)
        receive(5)
        compute(3)
        for r in range(roots):
            if end:
                ag_copy(r, chip).wait_recv()
            else:
                pl.when(chip != root_chip(r))(ag_copy(r, chip).wait_recv)
        last_swap(core).start()
        receive(6)
        compute(3)
        last_swap(1 - core).wait_recv()
        picked = jnp.concatenate([pick[c, r] for c in range(2) for r in range(roots)], axis=0)

        def part_rows(g):
            def go(i, _):
                rows = pl.ds(pl.multiple_of(i * TILE, TILE), TILE)
                source = pl.ds(pl.multiple_of(g * rows_of + i * TILE, TILE), TILE)
                parts[g, rows, :] = lax.dot_general(prior[source, :], picked, (((1,), (1,)), ((), ())), preferred_element_type=F32).astype(BF16)
                return 0
            lax.fori_loop(0, rows_of // TILE, go, 0)
        part_rows(1 - gy)
        part_rows(gy)
        receive(7)
        parts_copy().start()
        compute(3)
        for slot in range(8, slots + 1):
            receive(slot)
            if slot == slots:
                parts_copy().wait_recv()
                resid[...] = pair_ref[...] - (parts[gy].astype(F32) + parts_in[...].astype(F32))
            compute(3)
        compute(n)

        for copy in sent:
            copy.wait_send()
        parts_copy().wait_send()
        first_swap().wait_send()
        last_swap(core).wait_send()

        @pl.when(gy == 0)
        def _():
            for ch in range(chunks):
                slab_copy(ch).wait_send()
        for r in range(roots):
            if end:
                rs_copy(r, chip).wait_send()
            else:
                pl.when(chip != root_chip(r))(rs_copy(r, chip).wait_send)
        if not end:
            for step in range(1, chips):
                ag_copy(mine, lax.rem(chip + step, chips)).wait_send()

    pl.semaphore_wait(barrier, n)
    for me in range(2):
        pl.when(mirrored == me)(functools.partial(run, me))


def fused(n, old_block, vectors, prior, pair_columns, pivots):
    depth, width = vectors.shape[0], vectors.shape[2]
    rows, columns = old_block.shape
    keys, prior_width = pivots.shape[0], prior.shape[1]
    chips, roots = n // 2, 4
    each, chunks = keys // (2 * roots), width // TILE
    rows_of = prior.shape[0] // 2
    dma = pltpu.SemaphoreType.DMA
    anywhere = pl.BlockSpec(memory_space=pl.ANY)
    vmem = pl.BlockSpec(memory_space=pltpu.VMEM)
    acc, resid = pl.pallas_call(
        functools.partial(gather_kernel, n),
        out_shape=(pltpu.VMEM((rows, columns), F32), pltpu.VMEM(pair_columns.shape, F32)),
        in_specs=[anywhere, anywhere, anywhere, vmem, vmem],
        out_specs=(vmem, vmem),
        scratch_shapes=[
            pltpu.VMEM((n, chunks, depth, TILE), BF16),
            pltpu.VMEM((chunks, depth, TILE), BF16),
            pltpu.VMEM((width, depth), BF16),
            pltpu.VMEM(prior.shape, BF16),
            pltpu.VMEM((2, roots, each, prior_width), BF16),
            pltpu.VMEM((roots, each, prior_width), BF16),
            pltpu.VMEM((roots, each, prior_width), BF16),
            pltpu.VMEM((chips, each, prior_width), BF16),
            pltpu.VMEM((2, roots, each, prior_width), BF16),
            pltpu.VMEM((2, rows_of, keys), BF16),
            pltpu.VMEM((rows_of, keys), BF16),
            dma((chunks,)), dma, dma((n,)), dma((n, chunks, 4)), dma((n, chunks)), dma((chunks,)), dma((chunks,)), dma((2,)), dma((2,)),
            dma((roots,)), dma((chips,)), dma((chips,)), dma((roots,)), dma, dma,
        ],
        compiler_params=pltpu.CompilerParams(collective_id=0, has_side_effects=True, vmem_limit_bytes=VMEM_LIMIT),
    )(vectors.reshape(depth, width), prior, old_block, pair_columns, pivots.reshape(1, keys))
    return acc, resid


VMEM_LIMIT = 22 * 1024 * 1024


def solution(mesh):
    n, m = mesh.shape["gx"], mesh.shape["gy"]

    def local(old_block, vectors, prior, pair_columns, pivots):
        width = vectors.shape[2]
        whole_tiles = width % TILE == 0 and old_block.shape[0] % TILE == 0 and prior.shape[1] % TILE == 0 and prior.shape[0] // m % TILE == 0
        if n // 4 == 4 and n % 4 == 0 and m == 2 and pivots.shape[0] % 128 == 0 and whole_tiles:
            return fused(n, old_block, vectors, prior, pair_columns, pivots)
        return plain(old_block, vectors, prior, pair_columns, pivots)

    placed = (P("gx", "gy"), P(None, "gy", "gx"), P("gx", "gy"), P(("gx", "gy"), None), P())
    return jax.shard_map(
        local,
        mesh=mesh,
        in_specs=placed,
        out_specs=(P("gx", "gy"), P(("gx", "gy"), None)),
        check_vma=False,
    )
```

```python
import functools

import jax
import jax.numpy as jnp
from jax import lax
from jax.experimental import pallas as pl
from jax.experimental.pallas import tpu as pltpu
from jax.sharding import PartitionSpec as P

F32 = jnp.float32
BF16 = jnp.bfloat16
MESH = pl.DeviceIdType.MESH
TILE = 256


def from_root(value, axis, root):
    mine = lax.axis_index(axis) == root
    return lax.psum(jnp.where(mine, value, jnp.zeros_like(value)), axis)


def plain(old_block, vectors, prior, pair_columns, pivots):
    local_vectors = vectors.reshape(vectors.shape[0], vectors.shape[2])
    slab_part = from_root(local_vectors, "gy", 0)
    gained = jnp.dot(slab_part.T, lax.all_gather(local_vectors, "gx", axis=1, tiled=True), preferred_element_type=F32)
    new_block = old_block + gained
    rows_local = prior.shape[0]
    local_index = pivots - lax.axis_index("gx") * rows_local
    inside = jnp.logical_and(local_index >= 0, local_index < rows_local)
    chosen = jnp.take(prior, jnp.clip(local_index, 0, rows_local - 1), axis=0)
    chosen = jnp.where(inside[:, None], chosen, jnp.zeros_like(chosen))
    pivot_block = lax.psum(chosen, "gx")
    part = jnp.dot(prior, pivot_block.T, preferred_element_type=F32).astype(BF16)
    parts = lax.all_to_all(part.reshape(lax.axis_size("gy"), -1, part.shape[1]), "gy", split_axis=0, concat_axis=0)
    rounded = lax.optimization_barrier(parts)
    return new_block, pair_columns - jnp.sum(rounded.astype(F32), axis=0)


def gather_kernel(n, vec_ref, prior_ref, old_ref, pair_ref, piv_ref, acc, resid, held, slab, slab_t, prior, chosen, half_in,
                  half, rs_in, pick, parts, parts_in, vec_sem, prior_sem, old_sem, pair_sem, sends, v_recv, s_recv, d_recv,
                  rs_recv, ag_recv, p_recv, near_sem):
    line, chips = n // 4, n // 2
    chunks = held.shape[1]
    width = chunks * TILE
    keys = piv_ref.shape[1]
    roots, each = pick.shape[1], pick.shape[2]
    rows_of = prior.shape[0] // 2
    gx, gy = lax.axis_index("gx"), lax.axis_index("gy")
    pos, y, core = gx // 4, lax.rem(gx // 2, 2), lax.rem(gx, 2)
    chip = gx // 2
    flip = pos >= line // 2
    mirrored = jnp.where(flip, line - 1 - pos, pos)

    def at(k, yy, c):
        return (jnp.where(flip, line - 1 - k, k) * 2 + yy) * 2 + c

    def vec_copy(ch):
        return pltpu.make_async_copy(vec_ref.at[:, pl.ds(ch * TILE, TILE)], held.at[gx, ch], vec_sem.at[ch])

    for ch in range(chunks):
        vec_copy(ch).start()
    prior_in = pltpu.make_async_copy(prior_ref, prior, prior_sem)
    prior_in.start()
    pair_in = pltpu.make_async_copy(pair_ref, resid, pair_sem)
    pair_in.start()

    barrier = pltpu.get_barrier_semaphore()
    near = ((pos > 0, gx - 4), (pos < line - 1, gx + 4), (None, (pos * 2 + 1 - y) * 2 + core))

    def greet(sem):
        for ok, target in near:
            def go():
                pl.semaphore_signal(sem, inc=1, device_id=(target, gy), device_id_type=MESH)
            if ok is None:
                go()
            else:
                pl.when(ok)(go)

    greet(barrier)
    pl.semaphore_signal(barrier, inc=1, device_id=(chip * 2 + 1 - core, gy), device_id_type=MESH)
    pl.semaphore_signal(barrier, inc=1, device_id=(gx, 1 - gy), device_id_type=MESH)

    def old_copy(src):
        columns = pl.ds(pl.multiple_of(src * width, 128), width)
        return pltpu.make_async_copy(old_ref.at[:, columns], acc.at[:, columns], old_sem.at[src])

    def chunk_copy(src, ch, target):
        return pltpu.make_async_remote_copy(held.at[src, ch], held.at[src, ch], sends, v_recv.at[src, ch], device_id=(target, gy), device_id_type=MESH)

    def slab_copy(ch):
        return pltpu.make_async_remote_copy(held.at[gx, ch], slab.at[ch], sends, s_recv.at[ch], device_id=(gx, 1 - gy), device_id_type=MESH)

    partner = at(jnp.where(flip, line - 1 - pos, pos), y, 1 - core)

    def update(src, span):
        for ch in span:
            columns = pl.ds(pl.multiple_of(src * width + ch * TILE, TILE), TILE)
            acc[:, columns] += jnp.dot(slab_t[...], held[src, ch], preferred_element_type=F32)

    def first_swap():
        return pltpu.make_async_remote_copy(chosen.at[1 - core], half_in, sends, d_recv.at[0], device_id=(partner, gy), device_id_type=MESH)

    def last_swap(c):
        return pltpu.make_async_remote_copy(pick.at[c], pick.at[c], sends, d_recv.at[1], device_id=(partner, gy), device_id_type=MESH)

    def parts_copy():
        return pltpu.make_async_remote_copy(parts.at[1 - gy], parts_in, sends, p_recv, device_id=(gx, 1 - gy), device_id_type=MESH)

    def root_chip(r):
        return line // 2 * 2 - 2 + r

    def rs_copy(r, sender):
        return pltpu.make_async_remote_copy(half.at[r], rs_in.at[sender], sends, rs_recv.at[sender], device_id=(root_chip(r) * 2 + core, gy), device_id_type=MESH)

    def ag_copy(r, k):
        return pltpu.make_async_remote_copy(pick.at[core, r], pick.at[core, r], sends, ag_recv.at[r], device_id=(k * 2 + core, gy), device_id_type=MESH)

    def run(me):
        end = me == 0
        neighbours = 2 if end else 3
        pl.semaphore_wait(barrier, neighbours + 2)
        greet(near_sem.at[0])
        other = 1 - y
        sent = []

        def send(block, ch, way):
            k, own_y = block
            target = {"down": at(me - 1, y, core), "up": at(me + 1, y, core), "y": at(me, other, core), "core": partner}[way]
            copy = chunk_copy(at(k, y if own_y else other, core), ch, target)
            copy.start()
            sent.append(copy)

        def landed(block, ch, mine=True):
            k, own_y = block
            src = at(k, y if own_y else other, core if mine else 1 - core)
            chunk_copy(src, ch, gx).wait_recv()

        def ways(block, ch):
            k, own_y = block
            if end:
                out = []
                if block == (0, True):
                    out = ["y", "up"]
                elif block == (0, False):
                    out = ["up"]
                elif own_y and not (k == 3 and ch == chunks - 1):
                    out = ["y"]
                return out + ["core"]
            out = []
            if block == (1, True):
                out = ["down", "up", "y"]
            elif own_y and k > 1:
                out = ["down", "y"]
            elif block == (0, True):
                out = ["up"]
            elif block == (3, False) and ch == chunks - 1:
                out = ["down"]
            return out + ["core"]

        if end:
            from_z = [((k, True), c) for k in (1, 2, 3) for c in range(chunks)] + [((3, False), chunks - 1)]
            from_y = [((k, False), c) for k in range(line) for c in range(chunks)][:-1]
            streams = [from_z, from_y]
        else:
            streams = [
                [((2, True), c) for c in range(chunks)] + [((3, True), c) for c in range(chunks)],
                [((0, True), c) for c in range(chunks)] + [((0, False), c) for c in range(chunks)],
                [((k, False), c) for k in (1, 2, 3) for c in range(chunks)],
            ]
        slots = max(len(s) for s in streams)
        own = (me, True)

        def begin(ch, first):
            for way in ways(own, ch):
                if ch == 0 or (way == "up") != first:
                    send(own, ch, way)

        vec_copy(0).wait()
        begin(0, True)
        for ch in range(1, chunks):
            vec_copy(ch).wait()
            begin(ch, True)
        for ch in range(chunks):
            pl.when(gy == 0)(slab_copy(ch).start)
        prior_in.wait()
        pl.semaphore_wait(near_sem.at[0], neighbours)
        greet(near_sem.at[1])

        arrivals = [[(own, c) for c in range(chunks)]] + [[s[i] for s in streams if i < len(s)] for i in range(slots)]
        blocks = []
        for group in arrivals:
            for block, _ in group:
                if block not in blocks:
                    blocks.append(block)
        for k, own_y in blocks:
            for c in (core, 1 - core):
                old_copy(at(k, y if own_y else other, c)).start()

        got, ready, opened, late = {}, [], set(), []

        def note(block, ch, mine, slot):
            have = got.setdefault((block, mine), set())
            have.add(ch)
            if slot >= slots - 1:
                ready.extend((block, mine, c) for c in sorted(have))
                have.clear()
            elif len(have) == chunks:
                ready.append((block, mine, None))
                have.clear()

        def compute(budget):
            while ready and budget > 0:
                (k, own_y), mine, part = ready.pop(0)
                budget -= chunks if part is None else 1
                src = at(k, y if own_y else other, core if mine else 1 - core)
                span = range(chunks) if part is None else (part,)
                if not mine:
                    for ch in span:
                        landed((k, own_y), ch, False)
                if ((k, own_y), mine) not in opened:
                    opened.add(((k, own_y), mine))
                    old_copy(src).wait()
                update(src, span)

        def receive(slot):
            for block, ch in arrivals[slot]:
                landed(block, ch)
                for way in ways(block, ch):
                    send(block, ch, way)
            while late:
                note(*late.pop(0), slot)
            for block, ch in arrivals[slot]:
                note(block, ch, True, slot)
                late.append((block, ch, False))

        for ch in range(chunks):
            note(own, ch, True, 0)
        for ch in range(chunks):
            note(own, ch, False, 0)

        base = gx * prior.shape[0]
        key = jnp.broadcast_to(piv_ref[...], (keys, keys)).T
        key = key[:, :1] - base
        onehot = (lax.broadcasted_iota(jnp.int32, (keys, prior.shape[0]), 1) == key).astype(F32).astype(BF16)
        portion = keys // 2

        for i in range(prior.shape[1] // TILE):
            columns = slice(i * TILE, (i + 1) * TILE)
            got_rows = jnp.dot(onehot, prior[:, columns], preferred_element_type=F32).astype(BF16)
            for c in range(2):
                for r in range(roots):
                    start = c * portion + r * each
                    chosen[c, r, :, columns] = got_rows[start:start + each, :]

        first_swap().start()
        first_swap().wait_recv()
        for r in range(roots):
            half[r] = (chosen[core, r].astype(F32) + half_in[r].astype(F32)).astype(BF16)
        pl.semaphore_wait(near_sem.at[1], neighbours)
        for r in range(roots):
            if end:
                rs_copy(r, chip).start()
            else:
                pl.when(chip != root_chip(r))(rs_copy(r, chip).start)
        for ch in range(1, chunks):
            begin(ch, False)
        receive(1)
        receive(2)
        if not end:
            mine = chip - root_chip(0)
            total = half[mine].astype(F32)
            for step in range(1, chips):
                sender = lax.rem(chip + step, chips)
                rs_copy(0, sender).wait_recv()
                total = total + rs_in[sender].astype(F32)
            pick[core, mine] = total.astype(BF16)

        @pl.when(gy == 0)
        def _():
            for ch in range(chunks):
                slab_t[ch * TILE:(ch + 1) * TILE, :] = held[gx, ch].T

        @pl.when(gy != 0)
        def _():
            for ch in range(chunks):
                slab_copy(ch).wait_recv()
                slab_t[ch * TILE:(ch + 1) * TILE, :] = slab[ch].T

        if not end:
            for step in range(1, chips):
                ag_copy(mine, lax.rem(chip + step, chips)).start()
        receive(3)
        compute(6 if end else 0)
        receive(4)
        compute(6 if end else 0)
        receive(5)
        for r in range(roots):
            if end:
                ag_copy(r, chip).wait_recv()
            else:
                pl.when(chip != root_chip(r))(ag_copy(r, chip).wait_recv)
        last_swap(core).start()
        compute(6)
        last_swap(1 - core).wait_recv()
        picked = jnp.concatenate([pick[c, r] for c in range(2) for r in range(roots)], axis=0)

        def part_rows(g):
            source = pl.ds(pl.multiple_of(g * rows_of, TILE), rows_of)
            parts[g] = lax.dot_general(prior[source, :], picked, (((1,), (1,)), ((), ())), preferred_element_type=F32).astype(BF16)

        part_rows(1 - gy)
        receive(6)
        parts_copy().start()
        part_rows(gy)
        for slot in range(7, slots + 1):
            receive(slot)
            compute(8 if end else 6)
        while late:
            note(*late.pop(0), slots)
        compute(chunks * n)
        parts_copy().wait_recv()
        pair_in.wait()
        resid[...] -= parts[gy].astype(F32) + parts_in[...].astype(F32)

        for copy in sent:
            copy.wait_send()
        parts_copy().wait_send()
        first_swap().wait_send()
        last_swap(core).wait_send()

        @pl.when(gy == 0)
        def _():
            for ch in range(chunks):
                slab_copy(ch).wait_send()
        for r in range(roots):
            if end:
                rs_copy(r, chip).wait_send()
            else:
                pl.when(chip != root_chip(r))(rs_copy(r, chip).wait_send)
        if not end:
            for step in range(1, chips):
                ag_copy(mine, lax.rem(chip + step, chips)).wait_send()

    for me in range(2):
        pl.when(mirrored == me)(functools.partial(run, me))


def fused(n, old_block, vectors, prior, pair_columns, pivots):
    depth, width = vectors.shape[0], vectors.shape[2]
    rows, columns = old_block.shape
    keys, prior_width = pivots.shape[0], prior.shape[1]
    chips, roots = n // 2, 4
    each, chunks = keys // (2 * roots), width // TILE
    rows_of = prior.shape[0] // 2
    dma = pltpu.SemaphoreType.DMA
    anywhere = pl.BlockSpec(memory_space=pl.ANY)
    vmem = pl.BlockSpec(memory_space=pltpu.VMEM)
    acc, resid = pl.pallas_call(
        functools.partial(gather_kernel, n),
        out_shape=(pltpu.VMEM((rows, columns), F32), pltpu.VMEM(pair_columns.shape, F32)),
        in_specs=[anywhere, anywhere, anywhere, anywhere, vmem],
        out_specs=(vmem, vmem),
        scratch_shapes=[
            pltpu.VMEM((n, chunks, depth, TILE), BF16),
            pltpu.VMEM((chunks, depth, TILE), BF16),
            pltpu.VMEM((width, depth), BF16),
            pltpu.VMEM(prior.shape, BF16),
            pltpu.VMEM((2, roots, each, prior_width), BF16),
            pltpu.VMEM((roots, each, prior_width), BF16),
            pltpu.VMEM((roots, each, prior_width), BF16),
            pltpu.VMEM((chips, each, prior_width), BF16),
            pltpu.VMEM((2, roots, each, prior_width), BF16),
            pltpu.VMEM((2, rows_of, keys), BF16),
            pltpu.VMEM((rows_of, keys), BF16),
            dma((chunks,)), dma, dma((n,)), dma, dma, dma((n, chunks)), dma((chunks,)), dma((2,)),
            dma((chips,)), dma((roots,)), dma, pltpu.SemaphoreType.REGULAR((2,)),
        ],
        compiler_params=pltpu.CompilerParams(collective_id=0, has_side_effects=True, vmem_limit_bytes=VMEM_LIMIT),
    )(vectors.reshape(depth, width), prior, old_block, pair_columns, pivots.reshape(1, keys))
    return acc, resid


VMEM_LIMIT = 22 * 1024 * 1024


def solution(mesh):
    n, m = mesh.shape["gx"], mesh.shape["gy"]

    def local(old_block, vectors, prior, pair_columns, pivots):
        width = vectors.shape[2]
        whole_tiles = width % TILE == 0 and old_block.shape[0] % TILE == 0 and prior.shape[1] % TILE == 0 and prior.shape[0] // m % TILE == 0
        if n // 4 == 4 and n % 4 == 0 and m == 2 and pivots.shape[0] % 128 == 0 and whole_tiles:
            return fused(n, old_block, vectors, prior, pair_columns, pivots)
        return plain(old_block, vectors, prior, pair_columns, pivots)

    placed = (P("gx", "gy"), P(None, "gy", "gx"), P("gx", "gy"), P(("gx", "gy"), None), P())
    return jax.shard_map(
        local,
        mesh=mesh,
        in_specs=placed,
        out_specs=(P("gx", "gy"), P(("gx", "gy"), None)),
        check_vma=False,
    )
```

```python
import functools

import jax
import jax.numpy as jnp
from jax import lax
from jax.experimental import pallas as pl
from jax.experimental.pallas import tpu as pltpu
from jax.sharding import PartitionSpec as P

F32 = jnp.float32
BF16 = jnp.bfloat16
MESH = pl.DeviceIdType.MESH
TILE = 256


def from_root(value, axis, root):
    mine = lax.axis_index(axis) == root
    return lax.psum(jnp.where(mine, value, jnp.zeros_like(value)), axis)


def plain(old_block, vectors, prior, pair_columns, pivots):
    local_vectors = vectors.reshape(vectors.shape[0], vectors.shape[2])
    slab_part = from_root(local_vectors, "gy", 0)
    gained = jnp.dot(slab_part.T, lax.all_gather(local_vectors, "gx", axis=1, tiled=True), preferred_element_type=F32)
    new_block = old_block + gained
    rows_local = prior.shape[0]
    local_index = pivots - lax.axis_index("gx") * rows_local
    inside = jnp.logical_and(local_index >= 0, local_index < rows_local)
    chosen = jnp.take(prior, jnp.clip(local_index, 0, rows_local - 1), axis=0)
    chosen = jnp.where(inside[:, None], chosen, jnp.zeros_like(chosen))
    pivot_block = lax.psum(chosen, "gx")
    part = jnp.dot(prior, pivot_block.T, preferred_element_type=F32).astype(BF16)
    parts = lax.all_to_all(part.reshape(lax.axis_size("gy"), -1, part.shape[1]), "gy", split_axis=0, concat_axis=0)
    rounded = lax.optimization_barrier(parts)
    return new_block, pair_columns - jnp.sum(rounded.astype(F32), axis=0)


def gather_kernel(n, vec_ref, prior_ref, old_ref, pair_ref, piv_ref, acc, resid, held, slab, slab_t, prior, chosen, half_in,
                  half, rs_in, pick, parts, parts_in, vec_sem, prior_sem, old_sem, pair_sem, sends, v_recv, s_recv, d_recv,
                  rs_recv, ag_recv, p_recv, near_sem):
    line, chips = n // 4, n // 2
    chunks = held.shape[1]
    width = chunks * TILE
    keys = piv_ref.shape[1]
    roots, each = pick.shape[1], pick.shape[2]
    rows_of = prior.shape[0] // 2
    gx, gy = lax.axis_index("gx"), lax.axis_index("gy")
    pos, y, core = gx // 4, lax.rem(gx // 2, 2), lax.rem(gx, 2)
    chip = gx // 2
    flip = pos >= line // 2
    mirrored = jnp.where(flip, line - 1 - pos, pos)

    def at(k, yy, c):
        return (jnp.where(flip, line - 1 - k, k) * 2 + yy) * 2 + c

    def vec_copy(ch):
        return pltpu.make_async_copy(vec_ref.at[:, pl.ds(ch * TILE, TILE)], held.at[gx, ch], vec_sem.at[ch])

    for ch in range(chunks):
        vec_copy(ch).start()
    prior_in = pltpu.make_async_copy(prior_ref, prior, prior_sem)
    prior_in.start()
    pair_in = pltpu.make_async_copy(pair_ref, resid, pair_sem)
    pair_in.start()

    barrier = pltpu.get_barrier_semaphore()
    near = ((pos > 0, gx - 4), (pos < line - 1, gx + 4), (None, (pos * 2 + 1 - y) * 2 + core))

    def greet(sem):
        for ok, target in near:
            def go():
                pl.semaphore_signal(sem, inc=1, device_id=(target, gy), device_id_type=MESH)
            if ok is None:
                go()
            else:
                pl.when(ok)(go)

    greet(barrier)
    pl.semaphore_signal(barrier, inc=1, device_id=(chip * 2 + 1 - core, gy), device_id_type=MESH)
    pl.semaphore_signal(barrier, inc=1, device_id=(gx, 1 - gy), device_id_type=MESH)

    def old_copy(src):
        columns = pl.ds(pl.multiple_of(src * width, 128), width)
        return pltpu.make_async_copy(old_ref.at[:, columns], acc.at[:, columns], old_sem.at[src])

    def chunk_copy(src, ch, target):
        return pltpu.make_async_remote_copy(held.at[src, ch], held.at[src, ch], sends, v_recv.at[src, ch], device_id=(target, gy), device_id_type=MESH)

    def slab_copy(ch):
        return pltpu.make_async_remote_copy(held.at[gx, ch], slab.at[ch], sends, s_recv.at[ch], device_id=(gx, 1 - gy), device_id_type=MESH)

    partner = at(jnp.where(flip, line - 1 - pos, pos), y, 1 - core)

    def update(src, span):
        for ch in span:
            columns = pl.ds(pl.multiple_of(src * width + ch * TILE, TILE), TILE)
            acc[:, columns] += jnp.dot(slab_t[...], held[src, ch], preferred_element_type=F32)

    def first_swap():
        return pltpu.make_async_remote_copy(chosen.at[1 - core], half_in, sends, d_recv.at[0], device_id=(partner, gy), device_id_type=MESH)

    def last_swap(c):
        return pltpu.make_async_remote_copy(pick.at[c], pick.at[c], sends, d_recv.at[1], device_id=(partner, gy), device_id_type=MESH)

    def parts_copy():
        return pltpu.make_async_remote_copy(parts.at[1 - gy], parts_in, sends, p_recv, device_id=(gx, 1 - gy), device_id_type=MESH)

    def root_chip(r):
        return line // 2 * 2 - 2 + r

    def rs_copy(r, sender):
        return pltpu.make_async_remote_copy(half.at[r], rs_in.at[sender], sends, rs_recv.at[sender], device_id=(root_chip(r) * 2 + core, gy), device_id_type=MESH)

    def ag_copy(r, k):
        return pltpu.make_async_remote_copy(pick.at[core, r], pick.at[core, r], sends, ag_recv.at[r], device_id=(k * 2 + core, gy), device_id_type=MESH)

    def run(me):
        end = me == 0
        neighbours = 2 if end else 3
        pl.semaphore_wait(barrier, neighbours + 2)
        greet(near_sem.at[0])
        other = 1 - y
        sent = []

        def send(block, ch, way):
            k, own_y = block
            target = {"down": at(me - 1, y, core), "up": at(me + 1, y, core), "y": at(me, other, core), "core": partner}[way]
            copy = chunk_copy(at(k, y if own_y else other, core), ch, target)
            copy.start()
            sent.append(copy)

        def landed(block, ch, mine=True):
            k, own_y = block
            src = at(k, y if own_y else other, core if mine else 1 - core)
            chunk_copy(src, ch, gx).wait_recv()

        def ways(block, ch):
            k, own_y = block
            if end:
                out = []
                if block == (0, True):
                    out = ["y", "up"]
                elif block == (0, False):
                    out = ["up"]
                elif own_y and not (k == 3 and ch == 0):
                    out = ["y"]
                return out + ["core"]
            out = []
            if block == (1, True):
                out = ["down", "up", "y"]
            elif block == (3, True) and ch == 0:
                out = ["y"]
            elif own_y and k > 1:
                out = ["down", "y"]
            elif block == (0, True):
                out = ["up"]
            elif block == (3, False) and ch == 0:
                out = ["down"]
            return out + ["core"]

        if end:
            tail = [((3, True), c) for c in range(1, chunks)] + [((3, True), 0), ((3, False), 0)]
            from_z = [((k, True), c) for k in (1, 2) for c in range(chunks)] + tail
            from_y = [((k, False), c) for k in range(line) for c in range(chunks) if (k, c) != (3, 0)]
            streams = [from_z, from_y]
        else:
            streams = [
                [((2, True), c) for c in range(chunks)] + [((3, True), c) for c in range(chunks)],
                [((0, True), c) for c in range(chunks)] + [((0, False), c) for c in range(chunks)],
                [((k, False), c) for k in (1, 2, 3) for c in range(chunks)],
            ]
        slots = max(len(s) for s in streams)
        own = (me, True)

        def begin(ch):
            for way in ways(own, ch):
                send(own, ch, way)

        vec_copy(0).wait()
        begin(0)
        for ch in range(1, chunks):
            vec_copy(ch).wait()
            begin(ch)
        for ch in range(chunks):
            pl.when(gy == 0)(slab_copy(ch).start)
        prior_in.wait()
        pl.semaphore_wait(near_sem.at[0], neighbours)
        greet(near_sem.at[1])

        arrivals = [[(own, c) for c in range(chunks)]] + [[s[i] for s in streams if i < len(s)] for i in range(slots)]
        blocks = []
        for group in arrivals:
            for block, _ in group:
                if block not in blocks:
                    blocks.append(block)
        for k, own_y in blocks:
            for c in (core, 1 - core):
                old_copy(at(k, y if own_y else other, c)).start()

        got, ready, opened, late = {}, [], set(), []

        def note(block, ch, mine, slot):
            have = got.setdefault((block, mine), set())
            have.add(ch)
            if slot >= slots - 1:
                ready.extend((block, mine, c) for c in sorted(have))
                have.clear()
            elif len(have) == chunks:
                ready.append((block, mine, None))
                have.clear()

        def compute(budget):
            while ready and budget > 0:
                (k, own_y), mine, part = ready.pop(0)
                budget -= chunks if part is None else 1
                src = at(k, y if own_y else other, core if mine else 1 - core)
                span = range(chunks) if part is None else (part,)
                if not mine:
                    for ch in span:
                        landed((k, own_y), ch, False)
                if ((k, own_y), mine) not in opened:
                    opened.add(((k, own_y), mine))
                    old_copy(src).wait()
                update(src, span)

        def receive(slot):
            for block, ch in arrivals[slot]:
                landed(block, ch)
                for way in ways(block, ch):
                    send(block, ch, way)
                if not end and block == (3, True) and ch == chunks - 1:
                    send((3, True), 0, "down")
            while late:
                note(*late.pop(0), slot)
            for block, ch in arrivals[slot]:
                note(block, ch, True, slot)
                late.append((block, ch, False))

        for ch in range(chunks):
            note(own, ch, True, 0)
        for ch in range(chunks):
            note(own, ch, False, 0)

        base = gx * prior.shape[0]
        key = jnp.broadcast_to(piv_ref[...], (keys, keys)).T
        key = key[:, :1] - base
        onehot = (lax.broadcasted_iota(jnp.int32, (keys, prior.shape[0]), 1) == key).astype(F32).astype(BF16)
        portion = keys // 2

        for i in range(prior.shape[1] // TILE):
            columns = slice(i * TILE, (i + 1) * TILE)
            got_rows = jnp.dot(onehot, prior[:, columns], preferred_element_type=F32).astype(BF16)
            for c in range(2):
                for r in range(roots):
                    start = c * portion + r * each
                    chosen[c, r, :, columns] = got_rows[start:start + each, :]

        first_swap().start()
        first_swap().wait_recv()
        for r in range(roots):
            half[r] = (chosen[core, r].astype(F32) + half_in[r].astype(F32)).astype(BF16)
        pl.semaphore_wait(near_sem.at[1], neighbours)
        for r in range(roots):
            if end:
                rs_copy(r, chip).start()
            else:
                pl.when(chip != root_chip(r))(rs_copy(r, chip).start)
        receive(1)
        receive(2)
        if not end:
            mine = chip - root_chip(0)
            total = half[mine].astype(F32)
            for step in range(1, chips):
                sender = lax.rem(chip + step, chips)
                rs_copy(0, sender).wait_recv()
                total = total + rs_in[sender].astype(F32)
            pick[core, mine] = total.astype(BF16)

        @pl.when(gy == 0)
        def _():
            for ch in range(chunks):
                slab_t[ch * TILE:(ch + 1) * TILE, :] = held[gx, ch].T

        @pl.when(gy != 0)
        def _():
            for ch in range(chunks):
                slab_copy(ch).wait_recv()
                slab_t[ch * TILE:(ch + 1) * TILE, :] = slab[ch].T

        if not end:
            for step in range(1, chips):
                ag_copy(mine, lax.rem(chip + step, chips)).start()
        receive(3)
        compute(6)
        receive(4)
        compute(6)
        receive(5)
        compute(6)
        receive(6)
        compute(6)
        for r in range(roots):
            if end:
                ag_copy(r, chip).wait_recv()
            else:
                pl.when(chip != root_chip(r))(ag_copy(r, chip).wait_recv)
        last_swap(core).start()
        compute(6)
        last_swap(1 - core).wait_recv()
        picked = jnp.concatenate([pick[c, r] for c in range(2) for r in range(roots)], axis=0)

        def part_rows(g):
            source = pl.ds(pl.multiple_of(g * rows_of, TILE), rows_of)
            parts[g] = lax.dot_general(prior[source, :], picked, (((1,), (1,)), ((), ())), preferred_element_type=F32).astype(BF16)

        part_rows(1 - gy)
        receive(7)
        parts_copy().start()
        part_rows(gy)
        compute(6)
        for slot in range(8, slots + 1):
            receive(slot)
            compute(8)
        while late:
            note(*late.pop(0), slots)
        compute(chunks * n)
        parts_copy().wait_recv()
        pair_in.wait()
        resid[...] -= parts[gy].astype(F32) + parts_in[...].astype(F32)

        for copy in sent:
            copy.wait_send()
        parts_copy().wait_send()
        first_swap().wait_send()
        last_swap(core).wait_send()

        @pl.when(gy == 0)
        def _():
            for ch in range(chunks):
                slab_copy(ch).wait_send()
        for r in range(roots):
            if end:
                rs_copy(r, chip).wait_send()
            else:
                pl.when(chip != root_chip(r))(rs_copy(r, chip).wait_send)
        if not end:
            for step in range(1, chips):
                ag_copy(mine, lax.rem(chip + step, chips)).wait_send()

    for me in range(2):
        pl.when(mirrored == me)(functools.partial(run, me))


def fused(n, old_block, vectors, prior, pair_columns, pivots):
    depth, width = vectors.shape[0], vectors.shape[2]
    rows, columns = old_block.shape
    keys, prior_width = pivots.shape[0], prior.shape[1]
    chips, roots = n // 2, 4
    each, chunks = keys // (2 * roots), width // TILE
    rows_of = prior.shape[0] // 2
    dma = pltpu.SemaphoreType.DMA
    anywhere = pl.BlockSpec(memory_space=pl.ANY)
    vmem = pl.BlockSpec(memory_space=pltpu.VMEM)
    acc, resid = pl.pallas_call(
        functools.partial(gather_kernel, n),
        out_shape=(pltpu.VMEM((rows, columns), F32), pltpu.VMEM(pair_columns.shape, F32)),
        in_specs=[anywhere, anywhere, anywhere, anywhere, vmem],
        out_specs=(vmem, vmem),
        scratch_shapes=[
            pltpu.VMEM((n, chunks, depth, TILE), BF16),
            pltpu.VMEM((chunks, depth, TILE), BF16),
            pltpu.VMEM((width, depth), BF16),
            pltpu.VMEM(prior.shape, BF16),
            pltpu.VMEM((2, roots, each, prior_width), BF16),
            pltpu.VMEM((roots, each, prior_width), BF16),
            pltpu.VMEM((roots, each, prior_width), BF16),
            pltpu.VMEM((chips, each, prior_width), BF16),
            pltpu.VMEM((2, roots, each, prior_width), BF16),
            pltpu.VMEM((2, rows_of, keys), BF16),
            pltpu.VMEM((rows_of, keys), BF16),
            dma((chunks,)), dma, dma((n,)), dma, dma, dma((n, chunks)), dma((chunks,)), dma((2,)),
            dma((chips,)), dma((roots,)), dma, pltpu.SemaphoreType.REGULAR((2,)),
        ],
        compiler_params=pltpu.CompilerParams(collective_id=0, has_side_effects=True, vmem_limit_bytes=VMEM_LIMIT),
    )(vectors.reshape(depth, width), prior, old_block, pair_columns, pivots.reshape(1, keys))
    return acc, resid


VMEM_LIMIT = 22 * 1024 * 1024


def solution(mesh):
    n, m = mesh.shape["gx"], mesh.shape["gy"]

    def local(old_block, vectors, prior, pair_columns, pivots):
        width = vectors.shape[2]
        whole_tiles = width % TILE == 0 and old_block.shape[0] % TILE == 0 and prior.shape[1] % TILE == 0 and prior.shape[0] // m % TILE == 0
        if n // 4 == 4 and n % 4 == 0 and m == 2 and pivots.shape[0] % 128 == 0 and whole_tiles:
            return fused(n, old_block, vectors, prior, pair_columns, pivots)
        return plain(old_block, vectors, prior, pair_columns, pivots)

    placed = (P("gx", "gy"), P(None, "gy", "gx"), P("gx", "gy"), P(("gx", "gy"), None), P())
    return jax.shard_map(
        local,
        mesh=mesh,
        in_specs=placed,
        out_specs=(P("gx", "gy"), P(("gx", "gy"), None)),
        check_vma=False,
    )
```
